512 devices in a mesh: cols: 4 (over x), rows: 128 (over y, z, core).
Axes of the slice: x: 4, y: 8, z: 8, core: 2. Of those that a mesh axis runs over, the one named last changes fastest.
Arguments:
- gradient: float32 [128, 131072], P('cols', 'rows'), may hold values from -100 to 100
- width_factor: float32 [128, 128], P(None, 'cols'), may hold values from -3 to 4, as said below
- diag_blocks: float32 [1024, 128, 128], P('rows'), may hold values from -2 to 24, as said below
- jacobi_inverse: float32 [1024, 128, 128], P('rows'), may hold values from -2 to 2, as said below
- coupling_tiles: bfloat16 [8192, 128, 128], P('rows'), may hold values from -4 to 4, as said below
- tile_local: int32 [8192], P('rows'), may hold values from 0 to 7
- tile_remote: int32 [8192], P('rows'), may hold values from 0 to 1023, as said below
- tile_count: int32 [128], P('rows'), may hold values from 0 to 63, as said below
Outputs:
- solution: float32 [128, 131072], P('cols', 'rows')
- residual: float32 [128, 131072], P('cols', 'rows')
The draws below stay inside these ranges and needn't reach their ends.
Inputs may be any that keep to these rules, and one draw needn't show every extreme that they name: `tile_remote`: the live entries are the first tile_count entries of each device's list; they name distinct devices other than the owner, each at most once. For a live entry of device d naming block J of device e, device e has a live entry naming d's block with its tile the transpose. Pad entries hold valid indices. `tile_count`: at most 63 on one device, reached on some device. `coupling_tiles`: with diag_blocks and the live entries, M is symmetric positive definite. `diag_blocks`: symmetric positive definite tiles. `jacobi_inverse`: the inverses of diag_blocks, symmetric. `width_factor`: symmetric positive definite.
All inputs are finite; a program needn't handle non-finite values.
Results may differ from the reference program's by a relative error of at most 0.0085.
Values may be sent and summed in bfloat16 or wider, within the bound.
A program may use at most 64 MiB of HBM per device.

```python
import math
import jax
import jax.numpy as jnp
from jax import lax

WIDTH = 128
BLOCK = 128
BLOCKS_DEV = 8
ITERS = 6
OFFSETS = 32
SLOTS_DEV = 64
ALL_BLOCKS = 1024
ALL_ROWS = 131072
N_ROWS = 128


def layout(key):
    subkeys = jax.random.split(jax.random.fold_in(key, 7), 7)
    node_count = N_ROWS
    half_way = node_count // 2
    others = jax.random.permutation(subkeys[0], half_way - 2)[:OFFSETS - 2].astype(jnp.int32) + 2
    offsets = jnp.concatenate([jnp.array([1, half_way], dtype=jnp.int32), others])
    weights = jax.random.randint(subkeys[1], (node_count,), 0, 4)
    center = jax.random.randint(subkeys[2], (), 0, node_count)
    device = jnp.arange(node_count, dtype=jnp.int32)[:, None]
    slot_index = jnp.arange(OFFSETS, dtype=jnp.int32)[None, :]
    partner_up = (device + offsets[None, :]) % node_count
    partner_down = (device - offsets[None, :]) % node_count
    rolled = jax.random.randint(subkeys[3], (node_count, OFFSETS), 0, 8)
    random_live = (rolled < 2 + weights[:, None] + weights[partner_up]) | (device == center) | (partner_up == center)
    active = jnp.where(slot_index == 1, device < half_way, random_live)
    planted = slot_index < 2
    block_low = jax.random.randint(subkeys[4], (node_count, OFFSETS), 0, BLOCKS_DEV).astype(jnp.int32)
    block_high = jax.random.randint(subkeys[5], (node_count, OFFSETS), 0, BLOCKS_DEV).astype(jnp.int32)
    boost = jnp.where(planted, 8.0, 1.0)
    strength = boost * jnp.exp(jax.random.uniform(subkeys[6], (node_count, OFFSETS), minval=math.log(0.5), maxval=math.log(2.0))) / SLOTS_DEV
    is_live = jnp.concatenate([active, active[partner_down, slot_index]], axis=1)
    local_block = jnp.concatenate([block_low, block_high[partner_down, slot_index]], axis=1)
    remote = jnp.concatenate([partner_up * BLOCKS_DEV + block_high, partner_down * BLOCKS_DEV + block_low[partner_down, slot_index]], axis=1)
    edge_owner = jnp.concatenate([jnp.broadcast_to(device, (node_count, OFFSETS)), partner_down], axis=1)
    edge_slot = jnp.concatenate([jnp.broadcast_to(slot_index, (node_count, OFFSETS)), jnp.broadcast_to(slot_index, (node_count, OFFSETS))], axis=1)
    flipped = jnp.concatenate([jnp.zeros((node_count, OFFSETS), jnp.int32), jnp.ones((node_count, OFFSETS), jnp.int32)], axis=1)
    slot_strength = strength[edge_owner, edge_slot]
    matches = local_block[:, :, None] == jnp.arange(BLOCKS_DEV, dtype=jnp.int32)[None, None, :]
    shift_rows = jnp.sum((is_live.astype(jnp.float32) * 1.25 * slot_strength)[:, :, None] * matches.astype(jnp.float32), axis=1)
    compact_order = jnp.argsort(jnp.where(is_live, 0, 1), axis=1, stable=True)
    local_block = jnp.take_along_axis(local_block, compact_order, axis=1)
    remote = jnp.take_along_axis(remote, compact_order, axis=1)
    edge_owner = jnp.take_along_axis(edge_owner, compact_order, axis=1)
    edge_slot = jnp.take_along_axis(edge_slot, compact_order, axis=1)
    flipped = jnp.take_along_axis(flipped, compact_order, axis=1)
    live_count = jnp.sum(is_live.astype(jnp.int32), axis=1).astype(jnp.int32)
    return (local_block, remote, edge_owner, edge_slot, flipped, live_count, strength, shift_rows.reshape(ALL_BLOCKS))


def diagonal_matrix(key):
    shift_rows = layout(key)[7]
    entries = jax.random.uniform(jax.random.fold_in(key, 31), (ALL_BLOCKS, BLOCK, BLOCK), minval=-math.sqrt(3.0), maxval=math.sqrt(3.0))
    gram_matrix = jnp.einsum('nij,nkj->nik', entries, entries) / BLOCK
    identity = jnp.eye(BLOCK, dtype=jnp.float32)[None, :, :]
    matrix = 0.5 * identity + 0.5 * gram_matrix + shift_rows[:, None, None] * identity
    return 0.5 * (matrix + jnp.swapaxes(matrix, 1, 2))


def draw_diag_blocks(key, part):
    return diagonal_matrix(key).astype(jnp.float32)


def draw_jacobi_inverse(key, part):
    inverse = jnp.linalg.inv(diagonal_matrix(key))
    return (0.5 * (inverse + jnp.swapaxes(inverse, 1, 2))).astype(jnp.float32)


def draw_coupling_tiles(key, part):
    local_block, remote, edge_owner, edge_slot, flipped, live_count, strength, shift_rows = layout(key)
    raw_basis = jax.random.normal(jax.random.fold_in(key, 21), (N_ROWS, OFFSETS, BLOCK, BLOCK))
    orthogonal, upper_part = jnp.linalg.qr(raw_basis)
    scaled = (orthogonal * strength[:, :, None, None]).astype(jnp.bfloat16)
    picked = scaled[edge_owner, edge_slot]
    picked = jnp.where(flipped[:, :, None, None] == 1, jnp.swapaxes(picked, 2, 3), picked)
    return picked.reshape(N_ROWS * SLOTS_DEV, BLOCK, BLOCK)


def draw_tile_local(key, part):
    return layout(key)[0].reshape(N_ROWS * SLOTS_DEV).astype(jnp.int32)


def draw_tile_remote(key, part):
    return layout(key)[1].reshape(N_ROWS * SLOTS_DEV).astype(jnp.int32)


def draw_tile_count(key, part):
    return layout(key)[5].astype(jnp.int32)


def draw_width_factor(key, part):
    entries = jax.random.uniform(jax.random.fold_in(key, 41), (WIDTH, WIDTH), minval=-math.sqrt(3.0), maxval=math.sqrt(3.0))
    matrix = jnp.dot(entries, entries.T) / WIDTH + 0.05 * jnp.eye(WIDTH, dtype=jnp.float32)
    return (0.5 * (matrix + matrix.T)).astype(jnp.float32)


def draw_gradient(key, part):
    subkeys = jax.random.split(jax.random.fold_in(key, 51), 3)
    spread = math.log(math.sqrt(10.0))
    width_scale = jnp.exp(jax.random.uniform(subkeys[0], (WIDTH,), minval=-spread, maxval=spread))
    width_scale = width_scale * (1.0 + 2.0 * jnp.arange(WIDTH, dtype=jnp.float32) / WIDTH) / 2.0
    row_scale = jnp.exp(jax.random.uniform(subkeys[1], (ALL_ROWS,), minval=-spread, maxval=spread))
    row_scale = row_scale * (1.0 + 2.0 * jnp.arange(ALL_ROWS, dtype=jnp.float32) / ALL_ROWS) / 2.0
    core = jnp.clip(jax.random.normal(subkeys[2], (WIDTH, ALL_ROWS)), -4.0, 4.0)
    return (core * width_scale[:, None] * row_scale[None, :]).astype(jnp.float32)


def setup_inputs(seed: int = 0) -> dict:
    keys = jax.random.split(jax.random.key(seed), 9)
    return {
        "gradient": draw_gradient(jax.random.fold_in(keys[8], 71), 0),
        "width_factor": draw_width_factor(jax.random.fold_in(keys[8], 71), 0),
        "diag_blocks": draw_diag_blocks(jax.random.fold_in(keys[8], 71), 0),
        "jacobi_inverse": draw_jacobi_inverse(jax.random.fold_in(keys[8], 71), 0),
        "coupling_tiles": draw_coupling_tiles(jax.random.fold_in(keys[8], 71), 0),
        "tile_local": draw_tile_local(jax.random.fold_in(keys[8], 71), 0),
        "tile_remote": draw_tile_remote(jax.random.fold_in(keys[8], 71), 0),
        "tile_count": draw_tile_count(jax.random.fold_in(keys[8], 71), 0),
    }


highest = lax.Precision.HIGHEST

def coupling_sum(direction, coupling_tiles, tile_local, tile_remote, tile_count):
    barrier = lax.optimization_barrier(direction.astype(jnp.bfloat16))
    rounded = barrier.astype(jnp.float32).reshape(WIDTH, ALL_BLOCKS, BLOCK)
    tile_sets = coupling_tiles.reshape(N_ROWS, SLOTS_DEV, BLOCK, BLOCK)
    local_sets = tile_local.reshape(N_ROWS, SLOTS_DEV)
    remote_sets = tile_remote.reshape(N_ROWS, SLOTS_DEV)

    def one_device(inputs):
        tile_set, local_set, remote_set, live_count = inputs
        sources = rounded[:, remote_set, :]
        products = jnp.einsum('ekj,kji->eki', sources, tile_set.astype(jnp.float32), precision=highest)
        active_slot = jnp.arange(SLOTS_DEV, dtype=jnp.int32) < live_count
        placing = ((local_set[:, None] == jnp.arange(BLOCKS_DEV, dtype=jnp.int32)[None, :]) & active_slot[:, None]).astype(jnp.float32)
        return jnp.einsum('eki,kb->ebi', products, placing, precision=highest)
    pieces = lax.map(one_device, (tile_sets, local_sets, remote_sets, tile_count))
    return jnp.transpose(pieces, (1, 0, 2, 3)).reshape(WIDTH, ALL_ROWS)

def reference(gradient, width_factor, diag_blocks, jacobi_inverse, coupling_tiles, tile_local, tile_remote, tile_count):

    def apply_fisher(direction):
        blocks = direction.reshape(WIDTH, ALL_BLOCKS, BLOCK)
        local_part = jnp.einsum('enj,nji->eni', blocks, diag_blocks, precision=highest).reshape(WIDTH, ALL_ROWS)
        mixed_rows = local_part + coupling_sum(direction, coupling_tiles, tile_local, tile_remote, tile_count)
        return jnp.dot(width_factor, mixed_rows, precision=highest)

    def precondition(vector):
        blocks = vector.reshape(WIDTH, ALL_BLOCKS, BLOCK)
        return jnp.einsum('enj,nji->eni', blocks, jacobi_inverse, precision=highest).reshape(WIDTH, ALL_ROWS)
    solution = jnp.zeros_like(gradient)
    residual = gradient
    precond_res = precondition(residual)
    direction = precond_res
    res_norm = jnp.sum(residual * precond_res)
    for iteration in range(ITERS):
        fisher_dir = apply_fisher(direction)
        step_size = res_norm / jnp.sum(direction * fisher_dir)
        solution = solution + step_size * direction
        residual = residual - step_size * fisher_dir
        if iteration + 1 < ITERS:
            precond_res = precondition(residual)
            next_norm = jnp.sum(residual * precond_res)
            direction = precond_res + next_norm / res_norm * direction
            res_norm = next_norm
    return (solution, residual)
```

```python
import functools
import math

import jax
import jax.numpy as jnp
from jax import lax
from jax.experimental import pallas as pl
from jax.experimental.pallas import tpu as pltpu
from jax.sharding import PartitionSpec as P

BLOCK = 128
ITERS = 6
BLOCKS_DEV = 8
MESH = pl.DeviceIdType.MESH
f32, bf16 = jnp.float32, jnp.bfloat16


def dot(a, b):
    return jnp.dot(a, b, preferred_element_type=f32)


def split(v):
    high = v.astype(bf16)
    return high, (v - high.astype(f32)).astype(bf16)


def times_tile(v, high_ref, low_ref, n):
    width = v.shape[0]
    high, low = split(v)
    both = dot(jnp.concatenate([high, low], axis=0), high_ref[n])
    return both[:width] + both[width:] + dot(high, low_ref[n])


def kernel(
    nx, side, slots, width,
    local_s, remote_s, count_s, grad_ref, wt_ref, diag_ref, jac_ref, tiles_ref,
    sol_ref, res_ref,
    r, z, d, q, gz, xs, err, t, terr,
    jh, jl, dh, dl, wstack, wh, scal,
    grant_row, grant_got, grant_s, index0_s, index1_s, place_s,
    ag_snd, ag_even_y, ag_even_z, ag_odd_y, ag_odd_z,
    aa_snd, aa_even_y, aa_even_z, aa_odd_y, aa_odd_z, xd_snd, xd_got, xc_snd, xc_got,
    ra_snd, ra_got, rb_snd, rb_got, rc_snd, rc_got,
    g_ssem, g_rsem, g_csem, ag_ssem, ag_rsem, aa_ssem, aa_rsem, xd_ssem, xd_rsem,
    xc_ssem, xc_rsem, r_ssem, r_rsem,
):
    ag_got = ((ag_even_y, ag_even_z), (ag_odd_y, ag_odd_z))
    aa_got = ((aa_even_y, aa_even_z), (aa_odd_y, aa_odd_z))
    blocks = BLOCKS_DEV
    half = width // 2
    ring = 2 * side
    mx = lax.axis_index("cols")
    me = lax.axis_index("rows")
    y, zc = me // ring, me % ring
    zz, c = zc // 2, me % 2
    yc = y * 2 + c

    def along_y(i):
        return i * ring + zc

    def along_z(i):
        return y * ring + i * 2 + c

    def in_zc(i):
        return y * ring + i

    def in_yc(i):
        return (i // 2) * ring + zz * 2 + i % 2

    def push(src, dst, ssem, rsem, device):
        pltpu.make_async_remote_copy(
            src_ref=src, dst_ref=dst, send_sem=ssem, recv_sem=rsem,
            device_id=device, device_id_type=MESH,
        ).start()

    def await_sent(ref, sem):
        pltpu.make_async_remote_copy(
            src_ref=ref, dst_ref=ref, send_sem=sem, recv_sem=sem,
            device_id={"rows": me}, device_id_type=MESH,
        ).wait_send()

    def await_got(ref, sem):
        pltpu.make_async_remote_copy(
            src_ref=ref, dst_ref=ref, send_sem=sem, recv_sem=sem,
            device_id={"rows": me}, device_id_type=MESH,
        ).wait_recv()

    barrier = pltpu.get_barrier_semaphore()
    partners = 0
    for j in range(1, ring):
        pl.semaphore_signal(
            barrier, inc=1, device_id={"rows": in_zc((zc + j) % ring)}, device_id_type=MESH
        )
        partners += 1
    for j in range(1, side):
        for k in range(2):
            pl.semaphore_signal(
                barrier, inc=1, device_id={"rows": in_yc(((y + j) % side) * 2 + k)},
                device_id_type=MESH,
            )
            partners += 1
    for j in range(1, nx):
        pl.semaphore_signal(
            barrier, inc=1, device_id={"cols": (mx + j) % nx}, device_id_type=MESH
        )
        partners += 1

    lanes = lax.broadcasted_iota(jnp.int32, (1, 128), 1)
    row = jnp.zeros((1, 128), jnp.int32)
    count = count_s[0]
    for k in range(slots):
        live = k < count
        local = local_s[k]
        owner = remote_s[k] // blocks
        row = jnp.where(lanes == jnp.where(live, owner, -1), local, row)
        oy, ozc = owner // ring, owner % ring
        index0_s[k] = ozc * side + oy
        index1_s[k] = (oy * 2 + owner % 2) * side + ozc // 2
        placed = jnp.where(live, local, blocks)
        for n in range(blocks):
            place_s[k * blocks + n] = jnp.where(placed == n, 1.0, 0.0).astype(f32)
    grant_row[...] = row

    for n in range(blocks):
        high, low = split(jac_ref[n])
        jh[n] = high
        jl[n] = low
        high, low = split(diag_ref[n])
        dh[n] = high
        dl[n] = low
        start = grad_ref[:, n * BLOCK : (n + 1) * BLOCK]
        r[n] = start
        q[n] = start
        for ref in (z, d, gz, xs, err):
            ref[n] = jnp.zeros((width, BLOCK), f32)
    high, low = split(wt_ref[...])
    wh[...] = high
    wstack[...] = jnp.concatenate([high, low], axis=0)
    scal[...] = jnp.zeros((8, 128), f32)

    pl.semaphore_wait(barrier, partners)

    for j in range(1, side):
        i = (y + j) % side
        push(grant_row, grant_got.at[0, y], g_ssem.at[0], g_rsem.at[0], {"rows": along_y(i)})
        i = (zz + j) % side
        push(grant_row, grant_got.at[1, zz], g_ssem.at[1], g_rsem.at[1], {"rows": along_z(i)})
    grant_got[0, y] = row
    grant_got[1, zz] = row

    def sums(e_par, values):
        ra_snd[...] = values
        ra_got[e_par, zc] = values
        for j in range(1, ring):
            push(ra_snd, ra_got.at[e_par, zc], r_ssem.at[0], r_rsem.at[0, e_par],
                 {"rows": in_zc((zc + j) % ring)})

    def sums_y(e_par):
        await_got(ra_got.at[e_par, pl.ds(0, ring - 1)], r_rsem.at[0, e_par])
        total = ra_got[e_par, 0]
        for i in range(1, ring):
            total = total + ra_got[e_par, i]
        rb_snd[...] = total
        rb_got[e_par, y] = total
        for j in range(1, side):
            push(rb_snd, rb_got.at[e_par, y], r_ssem.at[1], r_rsem.at[1, e_par],
                 {"rows": along_y((y + j) % side)})

    def sums_x(e_par):
        await_got(rb_got.at[e_par, pl.ds(0, side - 1)], r_rsem.at[1, e_par])
        total = rb_got[e_par, 0]
        for i in range(1, side):
            total = total + rb_got[e_par, i]
        rc_snd[...] = total
        rc_got[e_par, mx] = total
        for j in range(1, nx):
            push(rc_snd, rc_got.at[e_par, mx], r_ssem.at[2], r_rsem.at[2, e_par],
                 {"cols": (mx + j) % nx})

    def sums_end(e_par):
        await_got(rc_got.at[e_par, pl.ds(0, nx - 1)], r_rsem.at[2, e_par])
        total = rc_got[e_par, 0]
        for i in range(1, nx):
            total = total + rc_got[e_par, i]
        await_sent(ra_got.at[e_par, pl.ds(0, ring - 1)], r_ssem.at[0])
        await_sent(rb_got.at[e_par, pl.ds(0, side - 1)], r_ssem.at[1])
        await_sent(rc_got.at[e_par, pl.ds(0, nx - 1)], r_ssem.at[2])
        lane_sum = jnp.sum(total, axis=1, keepdims=True)
        return jnp.broadcast_to(lane_sum, (8, 128))

    def inner(pairs):
        rows = []
        for a, b in pairs:
            part = jnp.zeros((8, 128), f32)
            for n in range(blocks):
                prod = a[n] * b[n]
                for s in range(0, width, 8):
                    part = part + prod[s : s + 8]
            rows.append(jnp.sum(part, axis=0, keepdims=True))
        rows.append(jnp.zeros((8 - len(rows), 128), f32))
        return jnp.concatenate(rows, axis=0)

    def step(e, par):
        first = e == 0
        scales = scal[...]
        norm, inverse = scales[0:1], scales[1:2]

        for n in range(blocks):
            tn = times_tile(q[n], jh, jl, n)
            t[n] = tn
            msg = (tn + err[n] * inverse).astype(bf16)
            terr[n] = msg.astype(f32) - tn
            ag_snd[0, n] = msg[:half]
            ag_snd[1, n] = msg[half:]
            ag_got[par][0][y, n] = msg[:half]
            ag_got[par][1][zz, n] = msg[half:]
        for j in range(1, side):
            push(ag_snd.at[0], ag_got[par][0].at[y], ag_ssem.at[0], ag_rsem.at[0, par],
                 {"rows": along_y((y + j) % side)})
            push(ag_snd.at[1], ag_got[par][1].at[zz], ag_ssem.at[1], ag_rsem.at[1, par],
                 {"rows": along_z((zz + j) % side)})

        sums(par, inner([(d, q), (q, z), (q, t)]))

        for n in range(blocks):
            part = times_tile(t[n], dh, dl, n)
            xd_snd[n] = part
            xd_got[par, mx, n] = part
        for j in range(1, nx):
            push(xd_snd, xd_got.at[par, mx], xd_ssem, xd_rsem.at[par], {"cols": (mx + j) % nx})

        sums_y(par)

        for o in range(2):
            await_got(ag_got[par][o].at[pl.ds(0, side - 1)], ag_rsem.at[o, par])
            for i in range(ring):
                column = in_zc(i) if o == 0 else in_yc(i)
                for s in range(side):
                    aa_snd[o, i, s] = ag_got[par][o][s, grant_s[o, s, 0, column]]
            mine = zc if o == 0 else yc
            for j in range(1, ring):
                i = (mine + j) % ring
                push(aa_snd.at[o, i], aa_got[par][o].at[pl.ds(mine * side, side)],
                     aa_ssem.at[o], aa_rsem.at[o, par],
                     {"rows": in_zc(i) if o == 0 else in_yc(i)})
            for s in range(side):
                aa_got[par][o][mine * side + s] = aa_snd[o, mine, s]

        sums_x(par)
        total = sums_end(par)
        curvature, cross, second = total[0:1], total[1:2], total[2:3]
        size = norm / curvature
        following = norm - 2.0 * size * cross + size * size * second
        a = jnp.where(first, -1.0, size)
        a_res = jnp.where(first, 0.0, size)
        b = jnp.where(first, 0.0, following / norm)
        scal[0:1] = jnp.where(first, second, following)
        scal[1:2] = jnp.where(first, 0.0, 1.0 / a)
        for n in range(blocks):
            dn = d[n]
            xs[n] = xs[n] + a * dn
            r[n] = r[n] - a_res * q[n]
            zn = z[n] - a * t[n]
            z[n] = zn
            d[n] = zn + b * dn
            err[n] = err[n] - a * terr[n]

        for o in range(2):
            await_got(aa_got[par][o].at[pl.ds(0, (ring - 1) * side)], aa_rsem.at[o, par])

        unroll = 16

        def tiles(group, sums_of):
            sums_of = list(sums_of)
            for u in range(unroll):
                k = group * unroll + u
                source = jnp.concatenate(
                    [aa_got[par][0][index0_s[k]], aa_got[par][1][index1_s[k]]], axis=0
                )
                prod = dot(source, tiles_ref[k])
                for n in range(blocks):
                    sums_of[n] = sums_of[n] + place_s[k * blocks + n] * prod
            return tuple(sums_of)

        zero = jnp.zeros((width, BLOCK), f32)
        coupled = lax.fori_loop(0, slots // unroll, tiles, (zero,) * blocks)
        for n in range(blocks):
            part = coupled[n].astype(bf16)
            xc_snd[n] = part
            xc_got[par, mx, n] = part
        for j in range(1, nx):
            push(xc_snd, xc_got.at[par, mx], xc_ssem, xc_rsem.at[par], {"cols": (mx + j) % nx})
        await_got(xd_got.at[par, pl.ds(0, nx - 1)], xd_rsem.at[par])
        await_got(xc_got.at[par, pl.ds(0, nx - 1)], xc_rsem.at[par])

        for n in range(blocks):
            mixed = jnp.concatenate(
                [xd_got[par, i, n] + xc_got[par, i, n].astype(f32) for i in range(nx)], axis=0
            )
            high, low = split(mixed)
            both = dot(wstack[...], high)
            image = both[:width] + both[width:] + dot(wh[...], low)
            gn = gz[n] - a * image
            gz[n] = gn
            q[n] = gn + b * q[n]

        for o in range(2):
            await_sent(ag_got[par][o].at[pl.ds(0, side - 1)], ag_ssem.at[o])
            await_sent(aa_got[par][o].at[pl.ds(0, (ring - 1) * side)], aa_ssem.at[o])
        await_sent(xd_got.at[par, pl.ds(0, nx - 1)], xd_ssem)
        await_sent(xc_got.at[par, pl.ds(0, nx - 1)], xc_ssem)

    for o in range(2):
        await_got(grant_got.at[o, pl.ds(0, side - 1)], g_rsem.at[o])
        await_sent(grant_got.at[o, pl.ds(0, side - 1)], g_ssem.at[o])
    tables = pltpu.make_async_copy(grant_got, grant_s, g_csem)
    tables.start()
    tables.wait()

    def two_steps(i, carry):
        step(2 * i, 0)
        step(2 * i + 1, 1)
        return carry

    lax.fori_loop(0, ITERS // 2, two_steps, 0)

    par = ITERS % 2
    sums(par, inner([(d, q)]))
    sums_y(par)
    sums_x(par)
    total = sums_end(par)
    a = scal[0:1] / total[0:1]
    for n in range(blocks):
        sol_ref[:, n * BLOCK : (n + 1) * BLOCK] = xs[n] + a * d[n]
        res_ref[:, n * BLOCK : (n + 1) * BLOCK] = r[n] - a * q[n]


def on_device(
    gradient, width_factor, diag_blocks, jacobi_inverse, coupling_tiles, tile_local, tile_remote, tile_count,
):
    nx, rows = lax.axis_size("cols"), lax.axis_size("rows")
    side = math.isqrt(rows // 2)
    ring = 2 * side
    width = gradient.shape[0]
    slots = tile_local.shape[0]
    blocks = BLOCKS_DEV
    half = width // 2
    vmem = pl.BlockSpec(memory_space=pltpu.VMEM)
    smem = pl.BlockSpec(memory_space=pltpu.SMEM)
    state = pltpu.VMEM((blocks, width, BLOCK), f32)
    tile_set = pltpu.VMEM((blocks, BLOCK, BLOCK), bf16)
    sem = pltpu.SemaphoreType.DMA
    scratch = [
        *[state] * 9,
        *[tile_set] * 4,
        pltpu.VMEM((2 * width, nx * width), bf16),
        pltpu.VMEM((width, nx * width), bf16),
        pltpu.VMEM((8, 128), f32),
        pltpu.VMEM((1, 128), jnp.int32),
        pltpu.VMEM((2, side, 1, 128), jnp.int32),
        pltpu.SMEM((2, side, 1, 128), jnp.int32),
        pltpu.SMEM((slots,), jnp.int32),
        pltpu.SMEM((slots,), jnp.int32),
        pltpu.SMEM((slots * blocks,), f32),
        pltpu.VMEM((2, blocks, half, BLOCK), bf16),
        *[pltpu.VMEM((side, blocks, half, BLOCK), bf16)] * 4,
        pltpu.VMEM((2, ring, side, half, BLOCK), bf16),
        *[pltpu.VMEM((ring * side, half, BLOCK), bf16)] * 4,
        state,
        pltpu.VMEM((2, nx, blocks, width, BLOCK), f32),
        pltpu.VMEM((blocks, width, BLOCK), bf16),
        pltpu.VMEM((2, nx, blocks, width, BLOCK), bf16),
        pltpu.VMEM((8, 128), f32),
        pltpu.VMEM((2, ring, 8, 128), f32),
        pltpu.VMEM((8, 128), f32),
        pltpu.VMEM((2, side, 8, 128), f32),
        pltpu.VMEM((8, 128), f32),
        pltpu.VMEM((2, nx, 8, 128), f32),
        sem((2,)), sem((2,)), sem,
        sem((2,)), sem((2, 2)),
        sem((2,)), sem((2, 2)),
        sem, sem((2,)),
        sem, sem((2,)),
        sem((3,)), sem((3, 2)),
    ]
    return pl.pallas_call(
        functools.partial(kernel, nx, side, slots, width),
        out_shape=(jax.ShapeDtypeStruct(gradient.shape, f32),) * 2,
        in_specs=[smem, smem, smem] + [vmem] * 5,
        out_specs=(vmem, vmem),
        scratch_shapes=scratch,
        compiler_params=pltpu.CompilerParams(
            collective_id=0, has_side_effects=True, vmem_limit_bytes=40 * 2**20
        ),
    )(
        tile_local, tile_remote, tile_count,
        gradient, width_factor.T, diag_blocks, jacobi_inverse, coupling_tiles,
    )


def solution(mesh):
    placed = (
        P("cols", "rows"),
        P(None, "cols"),
        P("rows", None, None),
        P("rows", None, None),
        P("rows", None, None),
        P("rows"),
        P("rows"),
        P("rows"),
    )
    return jax.shard_map(
        on_device,
        mesh=mesh,
        in_specs=placed,
        out_specs=(P("cols", "rows"), P("cols", "rows")),
        check_vma=False,
    )
```

```python
import functools
import math

import jax
import jax.numpy as jnp
from jax import lax
from jax.experimental import pallas as pl
from jax.experimental.pallas import tpu as pltpu
from jax.sharding import PartitionSpec as P

BLOCK = 128
ITERS = 6
BLOCKS_DEV = 8
MESH = pl.DeviceIdType.MESH
f32, bf16 = jnp.float32, jnp.bfloat16


def dot(a, b):
    return jnp.dot(a, b, preferred_element_type=f32)


def split(v):
    high = v.astype(bf16)
    return high, (v - high.astype(f32)).astype(bf16)


def times_tile(v, high_ref, low_ref, n):
    width = v.shape[0]
    high, low = split(v)
    both = dot(jnp.concatenate([high, low], axis=0), high_ref[n])
    return both[:width] + both[width:] + dot(high, low_ref[n])


def kernel(
    nx, side, slots, width,
    local_s, remote_s, count_s, grad_hbm, wt_ref, diag_hbm, jac_hbm, tiles_hbm,
    sol_ref, res_ref,
    r, z, d, q, gz, xs, err, t, terr,
    grad_ref, diag_ref, jac_ref, tiles_ref,
    jh, jl, dh, dl, wstack, wh, scal,
    grant_row, grant_got, grant_s, index0_s, index1_s, place_s,
    ag_snd, near_even_y, near_even_z, near_odd_y, near_odd_z,
    far_even_y, far_even_z, far_odd_y, far_odd_z,
    aa_snd, aa_even_y, aa_even_z, aa_odd_y, aa_odd_z, xd_snd, xd_got, xc_snd, xc_got,
    ra_snd, ra_got, rb_snd, rb_got, rc_snd, rc_got,
    in_sem, g_ssem, g_rsem, g_csem, ag_ssem, ag_rsem, aa_ssem, aa_rsem, xd_ssem, xd_rsem,
    xc_ssem, xc_rsem, r_ssem, r_rsem,
):
    ag_got = (
        ((near_even_y, far_even_y), (near_even_z, far_even_z)),
        ((near_odd_y, far_odd_y), (near_odd_z, far_odd_z)),
    )
    aa_got = ((aa_even_y, aa_even_z), (aa_odd_y, aa_odd_z))
    blocks = BLOCKS_DEV
    half = width // 2
    ring = 2 * side
    mx = lax.axis_index("cols")
    me = lax.axis_index("rows")
    y, zc = me // ring, me % ring
    zz, c = zc // 2, me % 2
    yc = y * 2 + c
    reach = side // 4
    far_first = sorted(range(1, side), key=lambda j: -min(j, side - j))
    groups = (2 * reach + 1, side - 2 * reach - 1)
    starts = (0, 2 * reach + 1)

    inputs = [
        pltpu.make_async_copy(src, dst, in_sem.at[i])
        for i, (src, dst) in enumerate(
            ((jac_hbm, jac_ref), (diag_hbm, diag_ref), (grad_hbm, grad_ref), (tiles_hbm, tiles_ref))
        )
    ]
    for copy in inputs:
        copy.start()

    def along_y(i):
        return i * ring + zc

    def along_z(i):
        return y * ring + i * 2 + c

    def in_zc(i):
        return y * ring + i

    def in_yc(i):
        return (i // 2) * ring + zz * 2 + i % 2

    def push(src, dst, ssem, rsem, device):
        pltpu.make_async_remote_copy(
            src_ref=src, dst_ref=dst, send_sem=ssem, recv_sem=rsem,
            device_id=device, device_id_type=MESH,
        ).start()

    def await_sent(ref, sem):
        pltpu.make_async_remote_copy(
            src_ref=ref, dst_ref=ref, send_sem=sem, recv_sem=sem,
            device_id={"rows": me}, device_id_type=MESH,
        ).wait_send()

    def await_got(ref, sem):
        pltpu.make_async_remote_copy(
            src_ref=ref, dst_ref=ref, send_sem=sem, recv_sem=sem,
            device_id={"rows": me}, device_id_type=MESH,
        ).wait_recv()

    barrier = pltpu.get_barrier_semaphore()
    partners = 0
    for j in range(1, ring):
        pl.semaphore_signal(
            barrier, inc=1, device_id={"rows": in_zc((zc + j) % ring)}, device_id_type=MESH
        )
        partners += 1
    for j in range(1, side):
        for k in range(2):
            pl.semaphore_signal(
                barrier, inc=1, device_id={"rows": in_yc(((y + j) % side) * 2 + k)},
                device_id_type=MESH,
            )
            partners += 1
    for j in range(1, nx):
        pl.semaphore_signal(
            barrier, inc=1, device_id={"cols": (mx + j) % nx}, device_id_type=MESH
        )
        partners += 1

    lanes = lax.broadcasted_iota(jnp.int32, (1, 128), 1)
    row = jnp.zeros((1, 128), jnp.int32)
    count = count_s[0]
    for k in range(slots):
        live = k < count
        local = local_s[k]
        owner = remote_s[k] // blocks
        row = jnp.where(lanes == jnp.where(live, owner, -1), local, row)
        oy, ozc = owner // ring, owner % ring
        index0_s[k] = ozc * side + (oy - y + side + reach) % side
        index1_s[k] = (oy * 2 + owner % 2) * side + (ozc // 2 - zz + side + reach) % side
        placed = jnp.where(live, local, blocks)
        for n in range(blocks):
            place_s[k * blocks + n] = jnp.where(placed == n, 1.0, 0.0).astype(f32)
    grant_row[...] = row
    for copy in inputs[:3]:
        copy.wait()

    for n in range(blocks):
        high, low = split(jac_ref[n])
        jh[n] = high
        jl[n] = low
        high, low = split(diag_ref[n])
        dh[n] = high
        dl[n] = low
        start = grad_ref[:, n * BLOCK : (n + 1) * BLOCK]
        r[n] = start
        q[n] = start
        for ref in (z, d, gz, xs, err):
            ref[n] = jnp.zeros((width, BLOCK), f32)
    high, low = split(wt_ref[...])
    wh[...] = high
    wstack[...] = jnp.concatenate([high, low], axis=0)
    scal[...] = jnp.zeros((8, 128), f32)

    pl.semaphore_wait(barrier, partners)

    for j in range(1, side):
        i = (y + j) % side
        push(grant_row, grant_got.at[0, y], g_ssem.at[0], g_rsem.at[0], {"rows": along_y(i)})
        i = (zz + j) % side
        push(grant_row, grant_got.at[1, zz], g_ssem.at[1], g_rsem.at[1], {"rows": along_z(i)})
    grant_got[0, y] = row
    grant_got[1, zz] = row

    def sums(e_par, values):
        ra_snd[...] = values
        ra_got[e_par, zc] = values
        for j in range(1, ring):
            push(ra_snd, ra_got.at[e_par, zc], r_ssem.at[0], r_rsem.at[0, e_par],
                 {"rows": in_zc((zc + j) % ring)})

    def sums_y(e_par):
        await_got(ra_got.at[e_par, pl.ds(0, ring - 1)], r_rsem.at[0, e_par])
        total = ra_got[e_par, 0]
        for i in range(1, ring):
            total = total + ra_got[e_par, i]
        rb_snd[...] = total
        rb_got[e_par, y] = total
        for j in range(1, side):
            push(rb_snd, rb_got.at[e_par, y], r_ssem.at[1], r_rsem.at[1, e_par],
                 {"rows": along_y((y + j) % side)})

    def sums_x(e_par):
        await_got(rb_got.at[e_par, pl.ds(0, side - 1)], r_rsem.at[1, e_par])
        total = rb_got[e_par, 0]
        for i in range(1, side):
            total = total + rb_got[e_par, i]
        rc_snd[...] = total
        rc_got[e_par, mx] = total
        for j in range(1, nx):
            push(rc_snd, rc_got.at[e_par, mx], r_ssem.at[2], r_rsem.at[2, e_par],
                 {"cols": (mx + j) % nx})

    def sums_end(e_par):
        await_got(rc_got.at[e_par, pl.ds(0, nx - 1)], r_rsem.at[2, e_par])
        total = rc_got[e_par, 0]
        for i in range(1, nx):
            total = total + rc_got[e_par, i]
        await_sent(ra_got.at[e_par, pl.ds(0, ring - 1)], r_ssem.at[0])
        await_sent(rb_got.at[e_par, pl.ds(0, side - 1)], r_ssem.at[1])
        await_sent(rc_got.at[e_par, pl.ds(0, nx - 1)], r_ssem.at[2])
        lane_sum = jnp.sum(total, axis=1, keepdims=True)
        return jnp.broadcast_to(lane_sum, (8, 128))

    def inner(pairs):
        rows = []
        for a, b in pairs:
            part = jnp.zeros((8, 128), f32)
            for n in range(blocks):
                prod = a[n] * b[n]
                for s in range(0, width, 8):
                    part = part + prod[s : s + 8]
            rows.append(jnp.sum(part, axis=0, keepdims=True))
        rows.append(jnp.zeros((8 - len(rows), 128), f32))
        return jnp.concatenate(rows, axis=0)

    def await_ag(par, o, group, got):
        copies = groups[group] - (1 if group == 0 else 0)
        if copies:
            await_got(got.at[pl.ds(0, copies)], ag_rsem.at[o, group, par])

    def step(e, par):
        first = e == 0
        scales = scal[...]
        norm, inverse = scales[0:1], scales[1:2]

        for n in range(blocks):
            tn = times_tile(q[n], jh, jl, n)
            t[n] = tn
            msg = (tn + err[n] * inverse).astype(bf16)
            terr[n] = msg.astype(f32) - tn
            ag_snd[0, n] = msg[:half]
            ag_snd[1, n] = msg[half:]
            ag_got[par][0][0][reach, n] = msg[:half]
            ag_got[par][1][0][reach, n] = msg[half:]
        sums(par, inner([(d, q), (q, z), (q, t)]))
        for group in range(2):
            for off in far_first:
                slot = (off + reach) % side - starts[group]
                if 0 <= slot < groups[group]:
                    push(ag_snd.at[0], ag_got[par][0][group].at[slot],
                         ag_ssem.at[0, group], ag_rsem.at[0, group, par],
                         {"rows": along_y((y - off + side) % side)})
                    push(ag_snd.at[1], ag_got[par][1][group].at[slot],
                         ag_ssem.at[1, group], ag_rsem.at[1, group, par],
                         {"rows": along_z((zz - off + side) % side)})

        for n in range(blocks):
            part = times_tile(t[n], dh, dl, n)
            xd_snd[n] = part
            xd_got[par, mx, n] = part
        for j in range(1, nx):
            push(xd_snd, xd_got.at[par, mx], xd_ssem, xd_rsem.at[par], {"cols": (mx + j) % nx})

        sums_y(par)

        if par == 0:
            @pl.when(first)
            def _():
                for o in range(2):
                    await_got(grant_got.at[o, pl.ds(0, side - 1)], g_rsem.at[o])
                    await_sent(grant_got.at[o, pl.ds(0, side - 1)], g_ssem.at[o])
                tables = pltpu.make_async_copy(grant_got, grant_s, g_csem)
                tables.start()
                tables.wait()

        for group in range(2):
            size, start = groups[group], starts[group]
            for o in range(2):
                got = ag_got[par][o][group]
                await_ag(par, o, group, got)
                at = y if o == 0 else zz
                for i in range(ring):
                    column = in_zc(i) if o == 0 else in_yc(i)
                    for s in range(size):
                        source = (at + start + s - reach + side) % side
                        aa_snd[o, i, start + s] = got[s, grant_s[o, source, 0, column]]
                mine = zc if o == 0 else yc
                middle = zz if o == 0 else y
                to = [((middle + off) % side) * 2 + k for off in far_first for k in range(2)]
                for i in [*to, middle * 2 + 1 - c]:
                    push(aa_snd.at[o, i, pl.ds(start, size)],
                         aa_got[par][o].at[pl.ds(mine * side + start, size)],
                         aa_ssem.at[o, group], aa_rsem.at[o, group, par],
                         {"rows": in_zc(i) if o == 0 else in_yc(i)})
                for s in range(start, start + size):
                    aa_got[par][o][mine * side + s] = aa_snd[o, mine, s]

        sums_x(par)
        total = sums_end(par)
        curvature, cross, second = total[0:1], total[1:2], total[2:3]
        size = norm / curvature
        following = norm - 2.0 * size * cross + size * size * second
        a = jnp.where(first, -1.0, size)
        a_res = jnp.where(first, 0.0, size)
        b = jnp.where(first, 0.0, following / norm)
        scal[0:1] = jnp.where(first, second, following)
        scal[1:2] = jnp.where(first, 0.0, 1.0 / a)
        for n in range(blocks):
            dn = d[n]
            xs[n] = xs[n] + a * dn
            r[n] = r[n] - a_res * q[n]
            zn = z[n] - a * t[n]
            z[n] = zn
            d[n] = zn + b * dn
            err[n] = err[n] - a * terr[n]

        if par == 0:
            @pl.when(first)
            def _():
                inputs[3].wait()
        for o in range(2):
            for group in range(2):
                amount = (ring - 1) * groups[group]
                await_got(aa_got[par][o].at[pl.ds(0, amount)], aa_rsem.at[o, group, par])

        unroll = min(32, slots)

        def tiles(group, sums_of):
            sums_of = list(sums_of)
            for u in range(unroll):
                k = group * unroll + u
                source = jnp.concatenate(
                    [aa_got[par][0][index0_s[k]], aa_got[par][1][index1_s[k]]], axis=0
                )
                prod = dot(source, tiles_ref[k])
                for n in range(blocks):
                    sums_of[n] = sums_of[n] + place_s[k * blocks + n] * prod
            return tuple(sums_of)

        zero = jnp.zeros((width, BLOCK), f32)
        coupled = lax.fori_loop(0, slots // unroll, tiles, (zero,) * blocks)
        for n in range(blocks):
            part = coupled[n].astype(bf16)
            xc_snd[n] = part
            xc_got[par, mx, n] = part
        for j in sorted(range(1, nx), key=lambda j: -min(j, nx - j)):
            push(xc_snd, xc_got.at[par, mx], xc_ssem, xc_rsem.at[par], {"cols": (mx + j) % nx})
        await_got(xd_got.at[par, pl.ds(0, nx - 1)], xd_rsem.at[par])
        await_got(xc_got.at[par, pl.ds(0, nx - 1)], xc_rsem.at[par])

        for n in range(blocks):
            mixed = jnp.concatenate(
                [xd_got[par, i, n] + xc_got[par, i, n].astype(f32) for i in range(nx)], axis=0
            )
            high, low = split(mixed)
            both = dot(wstack[...], high)
            image = both[:width] + both[width:] + dot(wh[...], low)
            gn = gz[n] - a * image
            gz[n] = gn
            q[n] = gn + b * q[n]

        for o in range(2):
            for group in range(2):
                copies = groups[group] - (1 if group == 0 else 0)
                if copies:
                    await_sent(ag_got[par][o][group].at[pl.ds(0, copies)], ag_ssem.at[o, group])
                amount = (ring - 1) * groups[group]
                await_sent(aa_got[par][o].at[pl.ds(0, amount)], aa_ssem.at[o, group])
        await_sent(xd_got.at[par, pl.ds(0, nx - 1)], xd_ssem)
        await_sent(xc_got.at[par, pl.ds(0, nx - 1)], xc_ssem)

    def two_steps(i, carry):
        step(2 * i, 0)
        step(2 * i + 1, 1)
        return carry

    lax.fori_loop(0, ITERS // 2, two_steps, 0)

    par = ITERS % 2
    sums(par, inner([(d, q)]))
    sums_y(par)
    sums_x(par)
    total = sums_end(par)
    a = scal[0:1] / total[0:1]
    for n in range(blocks):
        sol_ref[:, n * BLOCK : (n + 1) * BLOCK] = xs[n] + a * d[n]
        res_ref[:, n * BLOCK : (n + 1) * BLOCK] = r[n] - a * q[n]


def on_device(
    gradient, width_factor, diag_blocks, jacobi_inverse, coupling_tiles, tile_local, tile_remote, tile_count,
):
    nx, rows = lax.axis_size("cols"), lax.axis_size("rows")
    side = math.isqrt(rows // 2)
    ring = 2 * side
    width = gradient.shape[0]
    slots = tile_local.shape[0]
    blocks = BLOCKS_DEV
    half = width // 2
    near = 2 * (side // 4) + 1
    vmem = pl.BlockSpec(memory_space=pltpu.VMEM)
    smem = pl.BlockSpec(memory_space=pltpu.SMEM)
    hbm = pl.BlockSpec(memory_space=pltpu.HBM)
    state = pltpu.VMEM((blocks, width, BLOCK), f32)
    tile_set = pltpu.VMEM((blocks, BLOCK, BLOCK), bf16)
    sem = pltpu.SemaphoreType.DMA
    scratch = [
        *[state] * 9,
        pltpu.VMEM(gradient.shape, f32),
        pltpu.VMEM((blocks, BLOCK, BLOCK), f32),
        pltpu.VMEM((blocks, BLOCK, BLOCK), f32),
        pltpu.VMEM((slots, BLOCK, BLOCK), bf16),
        *[tile_set] * 4,
        pltpu.VMEM((2 * width, nx * width), bf16),
        pltpu.VMEM((width, nx * width), bf16),
        pltpu.VMEM((8, 128), f32),
        pltpu.VMEM((1, 128), jnp.int32),
        pltpu.VMEM((2, side, 1, 128), jnp.int32),
        pltpu.SMEM((2, side, 1, 128), jnp.int32),
        pltpu.SMEM((slots,), jnp.int32),
        pltpu.SMEM((slots,), jnp.int32),
        pltpu.SMEM((slots * blocks,), f32),
        pltpu.VMEM((2, blocks, half, BLOCK), bf16),
        *[pltpu.VMEM((near, blocks, half, BLOCK), bf16)] * 4,
        *[pltpu.VMEM((side - near, blocks, half, BLOCK), bf16)] * 4,
        pltpu.VMEM((2, ring, side, half, BLOCK), bf16),
        *[pltpu.VMEM((ring * side, half, BLOCK), bf16)] * 4,
        state,
        pltpu.VMEM((2, nx, blocks, width, BLOCK), f32),
        pltpu.VMEM((blocks, width, BLOCK), bf16),
        pltpu.VMEM((2, nx, blocks, width, BLOCK), bf16),
        pltpu.VMEM((8, 128), f32),
        pltpu.VMEM((2, ring, 8, 128), f32),
        pltpu.VMEM((8, 128), f32),
        pltpu.VMEM((2, side, 8, 128), f32),
        pltpu.VMEM((8, 128), f32),
        pltpu.VMEM((2, nx, 8, 128), f32),
        sem((4,)), sem((2,)), sem((2,)), sem,
        sem((2, 2)), sem((2, 2, 2)),
        sem((2, 2)), sem((2, 2, 2)),
        sem, sem((2,)),
        sem, sem((2,)),
        sem((3,)), sem((3, 2)),
    ]
    return pl.pallas_call(
        functools.partial(kernel, nx, side, slots, width),
        out_shape=(jax.ShapeDtypeStruct(gradient.shape, f32),) * 2,
        in_specs=[smem, smem, smem, hbm, vmem, hbm, hbm, hbm],
        out_specs=(vmem, vmem),
        scratch_shapes=scratch,
        compiler_params=pltpu.CompilerParams(
            collective_id=0, has_side_effects=True, vmem_limit_bytes=40 * 2**20
        ),
    )(
        tile_local, tile_remote, tile_count,
        gradient, width_factor.T, diag_blocks, jacobi_inverse, coupling_tiles,
    )


def solution(mesh):
    placed = (
        P("cols", "rows"),
        P(None, "cols"),
        P("rows", None, None),
        P("rows", None, None),
        P("rows", None, None),
        P("rows"),
        P("rows"),
        P("rows"),
    )
    return jax.shard_map(
        on_device,
        mesh=mesh,
        in_specs=placed,
        out_specs=(P("cols", "rows"), P("cols", "rows")),
        check_vma=False,
    )
```

```python
import functools
import math

import jax
import jax.numpy as jnp
from jax import lax
from jax.experimental import pallas as pl
from jax.experimental.pallas import tpu as pltpu
from jax.sharding import PartitionSpec as P

BLOCK = 128
ITERS = 6
BLOCKS_DEV = 8
MESH = pl.DeviceIdType.MESH
f32, bf16 = jnp.float32, jnp.bfloat16


def dot(a, b):
    return jnp.dot(a, b, preferred_element_type=f32)


def split(v):
    high = v.astype(bf16)
    return high, (v - high.astype(f32)).astype(bf16)


def times_tile(v, high_ref, low_ref, n):
    width = v.shape[0]
    high, low = split(v)
    both = dot(jnp.concatenate([high, low], axis=0), high_ref[n])
    return both[:width] + both[width:] + dot(high, low_ref[n])


def kernel(
    nx, side, slots, width,
    local_s, remote_s, count_s, grad_hbm, wt_ref, diag_hbm, jac_hbm, tiles_hbm,
    sol_ref, res_ref,
    r, z, d, q, gz, xs, err, t, terr,
    grad_ref, diag_ref, jac_ref, tiles_ref,
    jh, jl, dh, dl, wstack, wh, scal,
    grant_row, grant_got, grant_s, index0_s, index1_s, place_s,
    ag_snd, near_even_y, near_even_z, near_odd_y, near_odd_z,
    far_even_y, far_even_z, far_odd_y, far_odd_z,
    aa_snd, aa_even_y, aa_even_z, aa_odd_y, aa_odd_z, xd_snd, xd_got, xc_snd, xc_got,
    ra_snd, ra_got, rb_snd, rb_got, rc_snd, rc_got,
    in_sem, g_ssem, g_rsem, g_csem, ag_ssem, ag_rsem, aa_ssem, aa_rsem, xd_ssem, xd_rsem,
    xc_ssem, xc_rsem, r_ssem, r_rsem,
):
    ag_got = (
        ((near_even_y, far_even_y), (near_even_z, far_even_z)),
        ((near_odd_y, far_odd_y), (near_odd_z, far_odd_z)),
    )
    aa_got = ((aa_even_y, aa_even_z), (aa_odd_y, aa_odd_z))
    blocks = BLOCKS_DEV
    half = width // 2
    ring = 2 * side
    mx = lax.axis_index("cols")
    me = lax.axis_index("rows")
    y, zc = me // ring, me % ring
    zz, c = zc // 2, me % 2
    yc = y * 2 + c
    reach = side // 4
    far_first = sorted(range(1, side), key=lambda j: -min(j, side - j))
    groups = (2 * reach + 1, side - 2 * reach - 1)
    starts = (0, 2 * reach + 1)

    inputs = [
        pltpu.make_async_copy(src, dst, in_sem.at[i])
        for i, (src, dst) in enumerate(
            ((jac_hbm, jac_ref), (diag_hbm, diag_ref), (grad_hbm, grad_ref), (tiles_hbm, tiles_ref))
        )
    ]
    for copy in inputs:
        copy.start()

    def along_y(i):
        return i * ring + zc

    def along_z(i):
        return y * ring + i * 2 + c

    def in_zc(i):
        return y * ring + i

    def in_yc(i):
        return (i // 2) * ring + zz * 2 + i % 2

    def push(src, dst, ssem, rsem, device):
        pltpu.make_async_remote_copy(
            src_ref=src, dst_ref=dst, send_sem=ssem, recv_sem=rsem,
            device_id=device, device_id_type=MESH,
        ).start()

    def await_sent(ref, sem):
        pltpu.make_async_remote_copy(
            src_ref=ref, dst_ref=ref, send_sem=sem, recv_sem=sem,
            device_id={"rows": me}, device_id_type=MESH,
        ).wait_send()

    def await_got(ref, sem):
        pltpu.make_async_remote_copy(
            src_ref=ref, dst_ref=ref, send_sem=sem, recv_sem=sem,
            device_id={"rows": me}, device_id_type=MESH,
        ).wait_recv()

    barrier = pltpu.get_barrier_semaphore()
    partners = 0
    for j in range(1, ring):
        pl.semaphore_signal(
            barrier, inc=1, device_id={"rows": in_zc((zc + j) % ring)}, device_id_type=MESH
        )
        partners += 1
    for j in range(1, side):
        for k in range(2):
            pl.semaphore_signal(
                barrier, inc=1, device_id={"rows": in_yc(((y + j) % side) * 2 + k)},
                device_id_type=MESH,
            )
            partners += 1
    for j in range(1, nx):
        pl.semaphore_signal(
            barrier, inc=1, device_id={"cols": (mx + j) % nx}, device_id_type=MESH
        )
        partners += 1

    lanes = lax.broadcasted_iota(jnp.int32, (1, 128), 1)
    row = jnp.zeros((1, 128), jnp.int32)
    count = count_s[0]
    for k in range(slots):
        live = k < count
        local = local_s[k]
        owner = remote_s[k] // blocks
        row = jnp.where(lanes == jnp.where(live, owner, -1), local, row)
        oy, ozc = owner // ring, owner % ring
        index0_s[k] = ozc * side + (oy - y + side + reach) % side
        index1_s[k] = (oy * 2 + owner % 2) * side + (ozc // 2 - zz + side + reach) % side
        placed = jnp.where(live, local, blocks)
        for n in range(blocks):
            place_s[k * blocks + n] = jnp.where(placed == n, 1.0, 0.0).astype(f32)
    grant_row[...] = row
    for copy in inputs[:3]:
        copy.wait()

    for n in range(blocks):
        high, low = split(jac_ref[n])
        jh[n] = high
        jl[n] = low
        high, low = split(diag_ref[n])
        dh[n] = high
        dl[n] = low
        start = grad_ref[:, n * BLOCK : (n + 1) * BLOCK]
        r[n] = start
        q[n] = start
        for ref in (z, d, gz, xs, err):
            ref[n] = jnp.zeros((width, BLOCK), f32)
    high, low = split(wt_ref[...])
    wh[...] = high
    wstack[...] = jnp.concatenate([high, low], axis=0)
    scal[...] = jnp.zeros((8, 128), f32)

    pl.semaphore_wait(barrier, partners)

    for j in range(1, side):
        i = (y + j) % side
        push(grant_row, grant_got.at[0, y], g_ssem.at[0], g_rsem.at[0], {"rows": along_y(i)})
        i = (zz + j) % side
        push(grant_row, grant_got.at[1, zz], g_ssem.at[1], g_rsem.at[1], {"rows": along_z(i)})
    grant_got[0, y] = row
    grant_got[1, zz] = row

    def sums(e_par, values):
        ra_snd[...] = values
        ra_got[e_par, zc] = values
        for j in range(1, ring):
            push(ra_snd, ra_got.at[e_par, zc], r_ssem.at[0], r_rsem.at[0, e_par],
                 {"rows": in_zc((zc + j) % ring)})

    def sums_y(e_par):
        await_got(ra_got.at[e_par, pl.ds(0, ring - 1)], r_rsem.at[0, e_par])
        total = ra_got[e_par, 0]
        for i in range(1, ring):
            total = total + ra_got[e_par, i]
        rb_snd[...] = total
        rb_got[e_par, y] = total
        for j in range(1, side):
            push(rb_snd, rb_got.at[e_par, y], r_ssem.at[1], r_rsem.at[1, e_par],
                 {"rows": along_y((y + j) % side)})

    def sums_x(e_par):
        await_got(rb_got.at[e_par, pl.ds(0, side - 1)], r_rsem.at[1, e_par])
        total = rb_got[e_par, 0]
        for i in range(1, side):
            total = total + rb_got[e_par, i]
        rc_snd[...] = total
        rc_got[e_par, mx] = total
        for j in range(1, nx):
            push(rc_snd, rc_got.at[e_par, mx], r_ssem.at[2], r_rsem.at[2, e_par],
                 {"cols": (mx + j) % nx})

    def sums_end(e_par):
        await_got(rc_got.at[e_par, pl.ds(0, nx - 1)], r_rsem.at[2, e_par])
        total = rc_got[e_par, 0]
        for i in range(1, nx):
            total = total + rc_got[e_par, i]
        await_sent(ra_got.at[e_par, pl.ds(0, ring - 1)], r_ssem.at[0])
        await_sent(rb_got.at[e_par, pl.ds(0, side - 1)], r_ssem.at[1])
        await_sent(rc_got.at[e_par, pl.ds(0, nx - 1)], r_ssem.at[2])
        lane_sum = jnp.sum(total, axis=1, keepdims=True)
        return jnp.broadcast_to(lane_sum, (8, 128))

    def inner(pairs):
        rows = []
        for a, b in pairs:
            part = jnp.zeros((8, 128), f32)
            for n in range(blocks):
                prod = a[n] * b[n]
                for s in range(0, width, 8):
                    part = part + prod[s : s + 8]
            rows.append(jnp.sum(part, axis=0, keepdims=True))
        rows.append(jnp.zeros((8 - len(rows), 128), f32))
        return jnp.concatenate(rows, axis=0)

    def await_ag(par, o, group, got):
        copies = groups[group] - (1 if group == 0 else 0)
        if copies:
            await_got(got.at[pl.ds(0, copies)], ag_rsem.at[o, group, par])

    def step(e, par):
        first = e == 0
        scales = scal[...]
        norm, inverse = scales[0:1], scales[1:2]

        for n in range(blocks):
            tn = times_tile(q[n], jh, jl, n)
            t[n] = tn
            msg = (tn + err[n] * inverse).astype(bf16)
            terr[n] = msg.astype(f32) - tn
            ag_snd[0, n] = msg[:half]
            ag_snd[1, n] = msg[half:]
            ag_got[par][0][0][reach, n] = msg[:half]
            ag_got[par][1][0][reach, n] = msg[half:]
        sums(par, inner([(d, q), (q, z), (q, t)]))
        for group in range(2):
            for off in far_first:
                slot = (off + reach) % side - starts[group]
                if 0 <= slot < groups[group]:
                    push(ag_snd.at[0], ag_got[par][0][group].at[slot],
                         ag_ssem.at[0, group], ag_rsem.at[0, group, par],
                         {"rows": along_y((y - off + side) % side)})
                    push(ag_snd.at[1], ag_got[par][1][group].at[slot],
                         ag_ssem.at[1, group], ag_rsem.at[1, group, par],
                         {"rows": along_z((zz - off + side) % side)})

        for n in range(blocks):
            part = times_tile(t[n], dh, dl, n)
            xd_snd[n] = part
            xd_got[par, mx, n] = part
        for j in range(1, nx):
            push(xd_snd, xd_got.at[par, mx], xd_ssem, xd_rsem.at[par], {"cols": (mx + j) % nx})

        sums_y(par)

        if par == 0:
            @pl.when(first)
            def _():
                for o in range(2):
                    await_got(grant_got.at[o, pl.ds(0, side - 1)], g_rsem.at[o])
                    await_sent(grant_got.at[o, pl.ds(0, side - 1)], g_ssem.at[o])
                tables = pltpu.make_async_copy(grant_got, grant_s, g_csem)
                tables.start()
                tables.wait()

        for group in range(2):
            size, start = groups[group], starts[group]
            for o in range(2):
                got = ag_got[par][o][group]
                await_ag(par, o, group, got)
                at = y if o == 0 else zz
                for i in range(ring):
                    column = in_zc(i) if o == 0 else in_yc(i)
                    for s in range(size):
                        source = (at + start + s - reach + side) % side
                        aa_snd[o, i, start + s] = got[s, grant_s[o, source, 0, column]]
                mine = zc if o == 0 else yc
                middle = zz if o == 0 else y
                to = [((middle + off) % side) * 2 + k for off in far_first for k in range(2)]
                for i in [*to, middle * 2 + 1 - c]:
                    push(aa_snd.at[o, i, pl.ds(start, size)],
                         aa_got[par][o].at[pl.ds(mine * side + start, size)],
                         aa_ssem.at[o, group], aa_rsem.at[o, group, par],
                         {"rows": in_zc(i) if o == 0 else in_yc(i)})
                for s in range(start, start + size):
                    aa_got[par][o][mine * side + s] = aa_snd[o, mine, s]

        sums_x(par)
        total = sums_end(par)
        curvature, cross, second = total[0:1], total[1:2], total[2:3]
        size = norm / curvature
        following = norm - 2.0 * size * cross + size * size * second
        a = jnp.where(first, -1.0, size)
        a_res = jnp.where(first, 0.0, size)
        b = jnp.where(first, 0.0, following / norm)
        scal[0:1] = jnp.where(first, second, following)
        scal[1:2] = jnp.where(first, 0.0, 1.0 / a)
        for n in range(blocks):
            dn = d[n]
            xs[n] = xs[n] + a * dn
            r[n] = r[n] - a_res * q[n]
            zn = z[n] - a * t[n]
            z[n] = zn
            d[n] = zn + b * dn
            err[n] = err[n] - a * terr[n]

        if par == 0:
            @pl.when(first)
            def _():
                inputs[3].wait()
        for o in range(2):
            for group in range(2):
                amount = (ring - 1) * groups[group]
                await_got(aa_got[par][o].at[pl.ds(0, amount)], aa_rsem.at[o, group, par])

        unroll = min(32, slots)

        def tiles(group, sums_of):
            sums_of = list(sums_of)
            for u in range(unroll):
                k = group * unroll + u
                source = jnp.concatenate(
                    [aa_got[par][0][index0_s[k]], aa_got[par][1][index1_s[k]]], axis=0
                )
                prod = dot(source, tiles_ref[k])
                for n in range(blocks):
                    sums_of[n] = sums_of[n] + place_s[k * blocks + n] * prod
            return tuple(sums_of)

        zero = jnp.zeros((width, BLOCK), f32)
        coupled = lax.fori_loop(0, slots // unroll, tiles, (zero,) * blocks)
        for n in range(blocks):
            part = coupled[n].astype(bf16)
            xc_snd[n] = part
            xc_got[par, mx, n] = part
        for j in sorted(range(1, nx), key=lambda j: -min(j, nx - j)):
            push(xc_snd, xc_got.at[par, mx], xc_ssem, xc_rsem.at[par], {"cols": (mx + j) % nx})
        await_got(xd_got.at[par, pl.ds(0, nx - 1)], xd_rsem.at[par])
        await_got(xc_got.at[par, pl.ds(0, nx - 1)], xc_rsem.at[par])

        for n in range(blocks):
            mixed = jnp.concatenate(
                [xd_got[par, i, n] + xc_got[par, i, n].astype(f32) for i in range(nx)], axis=0
            )
            high, low = split(mixed)
            both = dot(wstack[...], high)
            image = both[:width] + both[width:] + dot(wh[...], low)
            gn = gz[n] - a * image
            gz[n] = gn
            q[n] = gn + b * q[n]

        for o in range(2):
            for group in range(2):
                copies = groups[group] - (1 if group == 0 else 0)
                if copies:
                    await_sent(ag_got[par][o][group].at[pl.ds(0, copies)], ag_ssem.at[o, group])
                amount = (ring - 1) * groups[group]
                await_sent(aa_got[par][o].at[pl.ds(0, amount)], aa_ssem.at[o, group])
        await_sent(xd_got.at[par, pl.ds(0, nx - 1)], xd_ssem)
        await_sent(xc_got.at[par, pl.ds(0, nx - 1)], xc_ssem)

    def two_steps(i, carry):
        step(2 * i, 0)
        step(2 * i + 1, 1)
        return carry

    lax.fori_loop(0, ITERS // 2, two_steps, 0)

    par = ITERS % 2
    sums(par, inner([(d, q)]))
    sums_y(par)
    sums_x(par)
    total = sums_end(par)
    a = scal[0:1] / total[0:1]
    for n in range(blocks):
        sol_ref[:, n * BLOCK : (n + 1) * BLOCK] = xs[n] + a * d[n]
        res_ref[:, n * BLOCK : (n + 1) * BLOCK] = r[n] - a * q[n]


def on_device(
    gradient, width_factor, diag_blocks, jacobi_inverse, coupling_tiles, tile_local, tile_remote, tile_count,
):
    nx, rows = lax.axis_size("cols"), lax.axis_size("rows")
    side = math.isqrt(rows // 2)
    ring = 2 * side
    width = gradient.shape[0]
    slots = tile_local.shape[0]
    blocks = BLOCKS_DEV
    half = width // 2
    near = 2 * (side // 4) + 1
    vmem = pl.BlockSpec(memory_space=pltpu.VMEM)
    smem = pl.BlockSpec(memory_space=pltpu.SMEM)
    hbm = pl.BlockSpec(memory_space=pltpu.HBM)
    state = pltpu.VMEM((blocks, width, BLOCK), f32)
    tile_set = pltpu.VMEM((blocks, BLOCK, BLOCK), bf16)
    sem = pltpu.SemaphoreType.DMA
    scratch = [
        *[state] * 9,
        pltpu.VMEM(gradient.shape, f32),
        pltpu.VMEM((blocks, BLOCK, BLOCK), f32),
        pltpu.VMEM((blocks, BLOCK, BLOCK), f32),
        pltpu.VMEM((slots, BLOCK, BLOCK), bf16),
        *[tile_set] * 4,
        pltpu.VMEM((2 * width, nx * width), bf16),
        pltpu.VMEM((width, nx * width), bf16),
        pltpu.VMEM((8, 128), f32),
        pltpu.VMEM((1, 128), jnp.int32),
        pltpu.VMEM((2, side, 1, 128), jnp.int32),
        pltpu.SMEM((2, side, 1, 128), jnp.int32),
        pltpu.SMEM((slots,), jnp.int32),
        pltpu.SMEM((slots,), jnp.int32),
        pltpu.SMEM((slots * blocks,), f32),
        pltpu.VMEM((2, blocks, half, BLOCK), bf16),
        *[pltpu.VMEM((near, blocks, half, BLOCK), bf16)] * 4,
        *[pltpu.VMEM((side - near, blocks, half, BLOCK), bf16)] * 4,
        pltpu.VMEM((2, ring, side, half, BLOCK), bf16),
        *[pltpu.VMEM((ring * side, half, BLOCK), bf16)] * 4,
        state,
        pltpu.VMEM((2, nx, blocks, width, BLOCK), f32),
        pltpu.VMEM((blocks, width, BLOCK), bf16),
        pltpu.VMEM((2, nx, blocks, width, BLOCK), bf16),
        pltpu.VMEM((8, 128), f32),
        pltpu.VMEM((2, ring, 8, 128), f32),
        pltpu.VMEM((8, 128), f32),
        pltpu.VMEM((2, side, 8, 128), f32),
        pltpu.VMEM((8, 128), f32),
        pltpu.VMEM((2, nx, 8, 128), f32),
        sem((4,)), sem((2,)), sem((2,)), sem,
        sem((2, 2)), sem((2, 2, 2)),
        sem((2, 2)), sem((2, 2, 2)),
        sem, sem((2,)),
        sem, sem((2,)),
        sem((3,)), sem((3, 2)),
    ]
    return pl.pallas_call(
        functools.partial(kernel, nx, side, slots, width),
        out_shape=(jax.ShapeDtypeStruct(gradient.shape, f32),) * 2,
        in_specs=[smem, smem, smem, hbm, vmem, hbm, hbm, hbm],
        out_specs=(vmem, vmem),
        scratch_shapes=scratch,
        compiler_params=pltpu.CompilerParams(
            collective_id=0, has_side_effects=True, vmem_limit_bytes=67_043_328
        ),
    )(
        tile_local, tile_remote, tile_count,
        gradient, width_factor.T, diag_blocks, jacobi_inverse, coupling_tiles,
    )


def solution(mesh):
    placed = (
        P("cols", "rows"),
        P(None, "cols"),
        P("rows", None, None),
        P("rows", None, None),
        P("rows", None, None),
        P("rows"),
        P("rows"),
        P("rows"),
    )
    return jax.shard_map(
        on_device,
        mesh=mesh,
        in_specs=placed,
        out_specs=(P("cols", "rows"), P("cols", "rows")),
        check_vma=False,
    )
```
